32 devices in a mesh: dp: 8 (over y, x, core), expert: 4 (over z).
Axes of the slice: x: 2, y: 2, z: 4, core: 2. Of those that a mesh axis runs over, the one named last changes fastest.
Arguments:
- grad_out: bfloat16 [2048, 2048], P('dp', 'expert'), may hold values from -48 to 48
- saved_inputs: bfloat16 [2048, 2048], P('dp', 'expert'), may hold values from -6 to 6
- router_probs: float32 [4, 2048], P('expert', 'dp'), may hold values from 0 to 1, as said below
- chosen: int32 [4, 512], replicated, may hold values from 0 to 2047, as said below
- gate_pre: bfloat16 [4, 512, 7168], P('expert', None, 'dp'), may hold values from -6 to 6
- up_pre: bfloat16 [4, 512, 7168], P('expert', None, 'dp'), may hold values from -6 to 6
- w_down: bfloat16 [4, 7168, 2048], P('expert', 'dp'), may hold values from -0.0625 to 0.0625
- w_up: bfloat16 [4, 7168, 2048], P('expert', 'dp'), may hold values from -0.125 to 0.125
Outputs:
- grad_tokens: bfloat16 [2048, 2048], P('dp', 'expert')
- grad_logits: float32 [4, 2048], P('expert', 'dp')
- grad_down: bfloat16 [4, 7168, 2048], P('expert', 'dp')
- grad_up: bfloat16 [4, 7168, 2048], P('expert', 'dp')
- grad_gate_pre: bfloat16 [4, 512, 7168], P('expert', None, 'dp')
The draws below stay inside these ranges and needn't reach their ends.
Inputs may be any that keep to these rules, and one draw needn't show every extreme that they name: `chosen`: every row lists 512 different tokens in increasing order. Among the 256 consecutive tokens of one index of dp, an expert chooses at most 96, and every expert chooses exactly 96 from some index of dp. `router_probs`: each token's probabilities over the 4 experts are positive and sum to one.
All inputs are finite; a program needn't handle non-finite values.
Results may differ from the reference program's by a relative error of at most 0.04.
Values may be sent and summed in bfloat16 or wider, within the bound.
A program may use at most 64 MiB of HBM per device.

```python
import jax
import jax.numpy as jnp
from jax import lax

WIDTH = 2048
FF_UNITS = 7168
TOK_DEV = 256
EXPERTS = 4
TOKENS = 2048
SLOTS = 512
CAP = 96
N_DP = 8


def draw_router_probs(key, part):
    first_key = jax.random.fold_in(key, 0)
    logits = 1.5 * jax.random.normal(first_key, (EXPERTS, TOKENS), jnp.float32)
    return jax.nn.softmax(logits, axis=0).astype(jnp.float32)


def draw_chosen(key, part):
    shard_total = TOKENS // TOK_DEV
    tier_key, top_key, noise_key = jax.random.split(key, 3)
    tiers = jax.random.randint(tier_key, (EXPERTS, shard_total), 0, 3)
    favored = jax.random.randint(top_key, (EXPERTS,), 0, shard_total)
    shard_ids = jnp.arange(shard_total, dtype=jnp.int32)
    tiers = jnp.where(shard_ids[None, :] == favored[:, None], 3, tiers)
    noise = jax.random.randint(noise_key, (EXPERTS, shard_total, TOK_DEV), 0, 4096)
    local_ids = jnp.arange(TOK_DEV, dtype=jnp.int32)
    distinct = noise * TOK_DEV + local_ids[None, None, :]
    order = jnp.argsort(-distinct, axis=2, stable=True)
    ranks = jnp.argsort(order, axis=2, stable=True)
    eligible = ranks < CAP
    global_ids = jnp.arange(TOKENS, dtype=jnp.int32).reshape(1, shard_total, TOK_DEV)
    scores = (tiers[:, :, None] * 4096 + noise) * TOKENS + global_ids
    scores = jnp.where(eligible, scores, -1).reshape(EXPERTS, TOKENS)
    picked = lax.top_k(scores, SLOTS)[1]
    return jnp.sort(picked, axis=1).astype(jnp.int32)


def block_scale(key, extent, cuts, smallest, top_value):
    def one(dim, parts):
        steps = jax.random.uniform(jax.random.fold_in(jax.random.fold_in(key, 6), dim), (parts,), jnp.float32, smallest / len(cuts), top_value / len(cuts))
        return jnp.repeat(jnp.exp(steps), extent[dim] // parts).reshape((-1,) + (1,) * (len(extent) - dim - 1))

    factor_of = one(*cuts[0])
    for cut in cuts[1:]:
        factor_of = factor_of * one(*cut)
    return factor_of


def gaussian(key, extent, spread, reach, cuts=(), held_as=jnp.bfloat16):
    drawn = spread * jax.random.normal(key, extent, jnp.float32)
    if cuts:
        drawn = drawn * block_scale(key, extent, cuts, -0.22, 0.18)
    return jnp.clip(drawn, -reach, reach).astype(held_as)


def setup_inputs(seed: int = 0) -> dict:
    arg_keys = jax.random.split(jax.random.key(seed), 9)
    return {
        "grad_out": gaussian(arg_keys[0], (TOKENS, WIDTH), 8.0, 48.0, ((0, 8), (1, 4))),
        "saved_inputs": gaussian(arg_keys[1], (TOKENS, WIDTH), 1.0, 6.0, ((0, 8), (1, 4))),
        "router_probs": draw_router_probs(jax.random.fold_in(arg_keys[8], 71), 0),
        "chosen": draw_chosen(jax.random.fold_in(arg_keys[8], 71), 0),
        "gate_pre": gaussian(arg_keys[4], (EXPERTS, SLOTS, FF_UNITS), 1.0, 6.0, ((0, 4), (2, 8))),
        "up_pre": gaussian(arg_keys[5], (EXPERTS, SLOTS, FF_UNITS), 1.0, 6.0, ((0, 4), (2, 8))),
        "w_down": gaussian(arg_keys[6], (EXPERTS, FF_UNITS, WIDTH), FF_UNITS ** -0.5, 0.0625, ((0, 4), (1, 8))),
        "w_up": gaussian(arg_keys[7], (EXPERTS, FF_UNITS, WIDTH), WIDTH ** -0.5, 0.125, ((0, 4), (1, 8))),
    }


def expert_backward(operands):
    dout_rows, input_rows, gate_slot, gate_block, up_block, down_block, upw_block = operands
    gate_value = gate_block.astype(jnp.float32)
    up_value = up_block.astype(jnp.float32)
    sigmoid_gate = jax.nn.sigmoid(gate_value)
    active = gate_value * sigmoid_gate
    hidden = active * up_value
    raw_grad = lax.dot_general(dout_rows, down_block, (((1,), (1,)), ((), ())), preferred_element_type=jnp.float32)
    hid_grad = gate_slot.astype(jnp.float32)[:, None] * raw_grad
    up_grad = (hid_grad * active).astype(jnp.bfloat16)
    gate_grad = (hid_grad * up_value * sigmoid_gate * (1.0 + gate_value * (1.0 - sigmoid_gate))).astype(jnp.bfloat16)
    out_grad = gate_slot[:, None] * dout_rows
    grad_down = lax.dot_general(hidden.astype(jnp.bfloat16), out_grad, (((0,), (0,)), ((), ())), preferred_element_type=jnp.float32).astype(jnp.bfloat16)
    grad_up = lax.dot_general(up_grad, input_rows, (((0,), (0,)), ((), ())), preferred_element_type=jnp.float32).astype(jnp.bfloat16)
    unit_block = FF_UNITS // N_DP
    up_split = up_grad.astype(jnp.float32).reshape(SLOTS, N_DP, unit_block)
    weight_split = upw_block.astype(jnp.float32).reshape(N_DP, unit_block, WIDTH)
    partial_value = jnp.einsum("spu,puw->psw", up_split, weight_split, precision=lax.Precision.HIGHEST)
    rounded = lax.optimization_barrier(partial_value.astype(jnp.bfloat16))
    expert_dx = jnp.sum(rounded.astype(jnp.float32), axis=0)
    dot_split = jnp.sum((hidden * raw_grad).reshape(SLOTS, N_DP, unit_block), axis=2)
    dot_round = lax.optimization_barrier(dot_split.astype(jnp.bfloat16))
    slot_dots = jnp.sum(dot_round.astype(jnp.float32), axis=1)
    return expert_dx, slot_dots, grad_down, grad_up, gate_grad


def reference(grad_out, saved_inputs, router_probs, chosen, gate_pre, up_pre, w_down, w_up):
    dout_rows = grad_out[chosen]
    input_rows = saved_inputs[chosen]
    gate_slot = jnp.take_along_axis(router_probs, chosen, axis=1).astype(jnp.bfloat16)
    results = lax.map(expert_backward, (dout_rows, input_rows, gate_slot, gate_pre, up_pre, w_down, w_up))
    expert_dx, slot_dots, grad_down, grad_up, grad_gate_pre = results
    summed = jax.ops.segment_sum(expert_dx.reshape(-1, WIDTH), chosen.reshape(-1), num_segments=TOKENS)
    grad_tokens = summed.astype(jnp.bfloat16)
    expert_ids = jnp.arange(EXPERTS, dtype=jnp.int32)[:, None]
    gate_grad = jnp.zeros((EXPERTS, TOKENS), jnp.float32).at[expert_ids, chosen].set(slot_dots)
    router_sum = jnp.sum(router_probs * gate_grad, axis=0)
    grad_logits = router_probs * (gate_grad - router_sum[None, :])
    return grad_tokens, grad_logits, grad_down, grad_up, grad_gate_pre
```

```python
import functools

import jax
import jax.numpy as jnp
from jax import lax
from jax.experimental import pallas as pl
from jax.experimental.pallas import tpu as pltpu
from jax.sharding import PartitionSpec as P

LANES = 128
MESH = pl.DeviceIdType.MESH


def bit_orders(shards):
    bits = [1 << k for k in range(shards.bit_length() - 1)]
    return bits, [bits[:1] + bits[1:], bits[:1] + bits[:0:-1]]


def span(bits):
    found = [0]
    for bit in bits:
        found = found + [r | bit for r in found]
    return found


def entry_barrier(experts, bits):
    e = lax.axis_index("expert")
    d = lax.axis_index("dp")
    barrier = pltpu.get_barrier_semaphore()
    for k in range(1, experts):
        pl.semaphore_signal(barrier, inc=1, device_id={"expert": lax.rem(e + k, experts)}, device_id_type=MESH)
    for bit in bits:
        pl.semaphore_signal(barrier, inc=1, device_id={"dp": d ^ bit}, device_id_type=MESH)
    pl.semaphore_wait(barrier, experts - 1 + len(bits))


def dispatch_kernel(experts, shards, g_ref, i_ref, gate_ref, gbuf, ibuf, loc, a2a_s, a2a_r, ag_s, ag_r):
    e = lax.axis_index("expert")
    d = lax.axis_index("dp")
    wd = g_ref.shape[2]
    width = wd * experts
    half = width // 2
    bits, orders = bit_orders(shards)
    entry_barrier(experts, bits)
    kinds = ((g_ref, gbuf), (i_ref, ibuf))

    def cols(src):
        return pl.ds(pl.multiple_of(src * wd, LANES), wd)

    def exchange(kind, k):
        ref, buf = kinds[kind]
        return pltpu.make_async_remote_copy(
            src_ref=ref.at[lax.rem(e + k, experts)],
            dst_ref=buf.at[d, :, cols(e)],
            send_sem=a2a_s.at[kind, k],
            recv_sem=a2a_r.at[kind, k],
            device_id={"expert": lax.rem(e + k, experts)},
            device_id_type=MESH,
        )

    def arrival(kind, k):
        ref, buf = kinds[kind]
        src = lax.rem(e + experts - k, experts)
        return pltpu.make_async_remote_copy(
            src_ref=ref.at[src],
            dst_ref=buf.at[d, :, cols(src)],
            send_sem=a2a_s.at[kind, k],
            recv_sem=a2a_r.at[kind, k],
            device_id={"expert": src},
            device_id_type=MESH,
        )

    for kind in range(2):
        for k in range(1, experts):
            exchange(kind, k).start()
    locals_ = [
        pltpu.make_async_copy(g_ref.at[e], gbuf.at[d, :, cols(e)], loc.at[0]),
        pltpu.make_async_copy(i_ref.at[e], ibuf.at[d, :, cols(e)], loc.at[1]),
        pltpu.make_async_copy(gate_ref, gbuf.at[d, :, pl.ds(width, LANES)], loc.at[2]),
    ]
    for c in locals_:
        c.start()
    streams = []
    for kind in range(2):
        buf = kinds[kind][1]
        ends = (half, buf.shape[2] - half)
        for part in range(2):
            order = orders[part][1:] + orders[part][:1]
            streams.append((buf, pl.ds(part * half, ends[part]), order))

    def piece(n, r, t):
        buf, cut, order = streams[n]
        block = buf.at[d ^ r, :, cut]
        return pltpu.make_async_remote_copy(
            src_ref=block,
            dst_ref=block,
            send_sem=ag_s.at[n, r | order[t]],
            recv_sem=ag_r.at[n, r | order[t]],
            device_id={"dp": d ^ order[t]},
            device_id_type=MESH,
        )

    def landed(n, r):
        buf, cut, order = streams[n]
        block = buf.at[d ^ r, :, cut]
        return pltpu.make_async_remote_copy(
            src_ref=block,
            dst_ref=block,
            send_sem=ag_s.at[n, r],
            recv_sem=ag_r.at[n, r],
            device_id={"dp": d ^ order[0]},
            device_id_type=MESH,
        )

    started = []

    def forward(n, r, first):
        for t in range(first, len(bits)):
            piece(n, r, t).start()
            started.append((n, r, t))

    for kind in range(2):
        locals_[kind].wait()
        if kind == 0:
            locals_[2].wait()
        for k in range(1, experts):
            arrival(kind, k).wait_recv()
        for part in range(2):
            forward(2 * kind + part, 0, 0)
    for t in range(len(bits)):
        for n in range(4):
            order = streams[n][2]
            for r in span(order[:t]):
                got = r | order[t]
                landed(n, got).wait_recv()
                forward(n, got, t + 1)
    for n, r, t in started:
        piece(n, r, t).wait_send()
    for kind in range(2):
        for k in range(1, experts):
            exchange(kind, k).wait_send()


def return_kernel(experts, shards, dx_ref, dots_ref, gate_ref, obuf, own_ref, ra, rb, rd, sbuf, sem_s, sem_r, a2a_s, a2a_r):
    e = lax.axis_index("expert")
    d = lax.axis_index("dp")
    width = dx_ref.shape[2]
    half = width // 2
    wd = width // experts
    bits, orders = bit_orders(shards)
    entry_barrier(experts, bits)
    streams = (
        (dx_ref, pl.ds(0, half), orders[0], ra),
        (dx_ref, pl.ds(half, half), orders[1], rb),
        (dots_ref, pl.ds(0, LANES), orders[0], rd),
    )
    steps = len(bits)

    def slot(n, t, r):
        order = streams[n][2]
        before = sum(1 << (steps - 1 - q) for q in range(t))
        return before + span(order[t + 1 :]).index(r)

    def held(n, t, r):
        src, cut, order, buf = streams[n]
        if t == 0:
            return src.at[d ^ r, :, cut]
        return buf.at[slot(n, t - 1, r)]

    def piece(n, t, r):
        src, cut, order, buf = streams[n]
        place = slot(n, t, r)
        return pltpu.make_async_remote_copy(
            src_ref=held(n, t, r | order[t]),
            dst_ref=buf.at[place],
            send_sem=sem_s.at[n, place],
            recv_sem=sem_r.at[n, place],
            device_id={"dp": d ^ order[t]},
            device_id_type=MESH,
        )

    for r_index in range(1 << (steps - 1)):
        for n in range(3):
            order = streams[n][2]
            r = list(reversed(span(order[1:])))[r_index]
            piece(n, 0, r).start()
    finals = [None] * 3
    for t in range(steps):
        for r_index in range(1 << (steps - 1 - t)):
            for n in range(3):
                src, cut, order, buf = streams[n]
                r = list(reversed(span(order[t + 1 :])))[r_index]
                piece(n, t, r).wait_recv()
                place = slot(n, t, r)
                total = held(n, t, r)[...].astype(jnp.float32) + buf[place].astype(jnp.float32)
                if t == steps - 1:
                    finals[n] = total
                    if n < 2:
                        per = half // wd
                        for q in range(per):
                            sbuf[n * per + q, :, 0:wd] = total[:, q * wd : (q + 1) * wd].astype(jnp.bfloat16)
                else:
                    buf[place] = total.astype(jnp.bfloat16)
                    if r & order[t + 1]:
                        piece(n, t + 1, r ^ order[t + 1]).start()
    dots = finals[2]
    own_ref[...] = dots
    weighted = dots * gate_ref[...]
    high = weighted.astype(jnp.bfloat16)
    low = (weighted - high.astype(jnp.float32)).astype(jnp.bfloat16)
    lane = lax.broadcasted_iota(jnp.int32, high.shape, 1)
    extra = jnp.where(lane == 0, high.astype(jnp.float32), low.astype(jnp.float32)).astype(jnp.bfloat16)
    for q in range(experts):
        sbuf[q, :, wd : wd + LANES] = extra

    def exchange(k):
        to = lax.rem(e + k, experts)
        return pltpu.make_async_remote_copy(
            src_ref=sbuf.at[to],
            dst_ref=obuf.at[e],
            send_sem=a2a_s.at[k],
            recv_sem=a2a_r.at[k],
            device_id={"expert": to},
            device_id_type=MESH,
        )

    def arrival(k):
        src = lax.rem(e + experts - k, experts)
        return pltpu.make_async_remote_copy(
            src_ref=sbuf.at[src],
            dst_ref=obuf.at[src],
            send_sem=a2a_s.at[k],
            recv_sem=a2a_r.at[k],
            device_id={"expert": src},
            device_id_type=MESH,
        )

    for k in range(1, experts):
        exchange(k).start()
    obuf[e] = sbuf[e]
    for k in range(1, experts):
        arrival(k).wait_recv()
    for k in range(1, experts):
        exchange(k).wait_send()
    for n in range(3):
        for t in range(steps):
            for r in span(streams[n][2][t + 1 :]):
                piece(n, t, r).wait_send()


VMEM = pl.BlockSpec(memory_space=pltpu.VMEM)


def dispatch(experts, shards, sent_grad, sent_input, gate_rows):
    _, cap, wd = sent_grad.shape
    width = experts * wd
    return pl.pallas_call(
        functools.partial(dispatch_kernel, experts, shards),
        out_shape=(
            jax.ShapeDtypeStruct((shards, cap, width + LANES), jnp.bfloat16),
            jax.ShapeDtypeStruct((shards, cap, width), jnp.bfloat16),
        ),
        in_specs=[VMEM] * 3,
        out_specs=(VMEM, VMEM),
        scratch_shapes=[
            pltpu.SemaphoreType.DMA((3,)),
            pltpu.SemaphoreType.DMA((2, experts)),
            pltpu.SemaphoreType.DMA((2, experts)),
            pltpu.SemaphoreType.DMA((4, shards)),
            pltpu.SemaphoreType.DMA((4, shards)),
        ],
        compiler_params=pltpu.CompilerParams(collective_id=0, has_side_effects=True),
        name="dispatch",
    )(sent_grad, sent_input, gate_rows)


def give_back(experts, shards, dx, dots, gate_rows):
    _, cap, width = dx.shape
    wd = width // experts
    return pl.pallas_call(
        functools.partial(return_kernel, experts, shards),
        out_shape=(
            jax.ShapeDtypeStruct((experts, cap, wd + LANES), jnp.bfloat16),
            jax.ShapeDtypeStruct((cap, LANES), jnp.float32),
        ),
        in_specs=[VMEM] * 3,
        out_specs=(VMEM, VMEM),
        scratch_shapes=[
            pltpu.VMEM((shards - 1, cap, width // 2), jnp.bfloat16),
            pltpu.VMEM((shards - 1, cap, width // 2), jnp.bfloat16),
            pltpu.VMEM((shards - 1, cap, LANES), jnp.bfloat16),
            pltpu.VMEM((experts, cap, wd + LANES), jnp.bfloat16),
            pltpu.SemaphoreType.DMA((3, shards)),
            pltpu.SemaphoreType.DMA((3, shards)),
            pltpu.SemaphoreType.DMA((experts,)),
            pltpu.SemaphoreType.DMA((experts,)),
        ],
        compiler_params=pltpu.CompilerParams(collective_id=1, has_side_effects=True),
        name="give_back",
    )(dx, dots, gate_rows)


def dot_t(a, b):
    return lax.dot_general(a, b, (((0,), (0,)), ((), ())), preferred_element_type=jnp.float32)


def local(grad_out, saved_inputs, router_probs, chosen, gate_pre, up_pre, w_down, w_up):
    tok_dev, wd = grad_out.shape
    shards = lax.axis_size("dp")
    shard_index = lax.axis_index("dp")
    expert = lax.axis_index("expert")
    experts, slots = chosen.shape
    cap = 3 * slots // (2 * shards)
    width = wd * experts
    bf16 = jnp.bfloat16
    owners = chosen // tok_dev
    firsts = jnp.sum((owners < shard_index).astype(jnp.int32), axis=1)
    slot_iota = jnp.arange(slots, dtype=jnp.int32)
    place = slot_iota[None, :] - firsts[:, None]
    place = jnp.where(owners == shard_index, place, -1)
    hit = place[:, None, :] == jnp.arange(cap, dtype=jnp.int32)[None, :, None]
    local_rows = jnp.max(jnp.where(hit, (chosen - shard_index * tok_dev)[:, None, :], -1), axis=2)
    token_iota = jnp.arange(tok_dev, dtype=jnp.int32)
    picker = (local_rows.reshape(-1)[:, None] == token_iota[None, :]).astype(bf16)
    sent_grad = jnp.dot(picker, grad_out, preferred_element_type=jnp.float32).astype(bf16)
    sent_input = jnp.dot(picker, saved_inputs, preferred_element_type=jnp.float32).astype(bf16)
    own_rows = lax.dynamic_index_in_dim(local_rows, expert, 0, keepdims=False)
    probs = router_probs[0]
    own_hit = own_rows[:, None] == token_iota[None, :]
    gate_own = jnp.sum(jnp.where(own_hit, probs[None, :], 0.0), axis=1)
    gate_wide = jnp.broadcast_to(gate_own[:, None], (cap, LANES))
    gbuf, ibuf = dispatch(
        experts,
        shards,
        sent_grad.reshape(experts, cap, wd),
        sent_input.reshape(experts, cap, wd),
        gate_wide.astype(bf16),
    )
    rows_all = shards * cap
    gbuf = gbuf.reshape(rows_all, width + LANES)
    ibuf = ibuf.reshape(rows_all, width)
    chosen_row = lax.dynamic_index_in_dim(chosen, expert, 0, keepdims=False)
    row_owner = chosen_row // tok_dev
    before = jnp.sum((row_owner[None, :] < row_owner[:, None]).astype(jnp.int32), axis=1)
    slot_place = row_owner * cap + slot_iota - before
    compact = (slot_place[:, None] == jnp.arange(rows_all, dtype=jnp.int32)[None, :]).astype(bf16)
    packed = jnp.dot(compact, gbuf, preferred_element_type=jnp.float32).astype(bf16)
    dout = packed[:, :width]
    gate_slot = packed[:, width:][:, :1]
    gate_value = gate_pre[0].astype(jnp.float32)
    up_value = up_pre[0].astype(jnp.float32)
    sig = jax.nn.sigmoid(gate_value)
    active = gate_value * sig
    hidden = active * up_value
    raw_grad = lax.dot_general(dout, w_down[0], (((1,), (1,)), ((), ())), preferred_element_type=jnp.float32)
    dots = jnp.sum(hidden * raw_grad, axis=1)
    hid_grad = gate_slot.astype(jnp.float32) * raw_grad
    up_grad = (hid_grad * active).astype(bf16)
    gate_grad = (hid_grad * up_value * sig * (1.0 + gate_value * (1.0 - sig))).astype(bf16)
    up_pad = dot_t(compact, up_grad).astype(bf16)
    dx = jnp.dot(up_pad, w_up[0], preferred_element_type=jnp.float32).astype(bf16)
    dots_wide = jnp.broadcast_to(dots.astype(bf16)[:, None], (slots, LANES))
    dots_pad = dot_t(compact, dots_wide).astype(bf16)
    grad_down = dot_t(hidden.astype(bf16), gate_slot * dout).astype(bf16)
    grad_up = dot_t(up_pad, ibuf).astype(bf16)
    spread, dots_own = give_back(
        experts, shards, dx.reshape(shards, cap, width), dots_pad.reshape(shards, cap, LANES), gate_wide
    )
    spread = spread.reshape(experts * cap, wd + LANES)
    summed = dot_t(picker, spread)
    grad_tokens = summed[:, :wd].astype(bf16)
    router_sum = summed[:, wd] + summed[:, wd + 1]
    gate_tokens = jnp.sum(jnp.where(own_hit, dots_own[:, :1], 0.0), axis=0)
    grad_logits = (probs * (gate_tokens - router_sum))[None, :]
    return grad_tokens, grad_logits, grad_down[None], grad_up[None], gate_grad[None]


def solution(mesh):
    in_specs = (
        P("dp", "expert"),
        P("dp", "expert"),
        P("expert", "dp"),
        P(),
        P("expert", None, "dp"),
        P("expert", None, "dp"),
        P("expert", "dp", None),
        P("expert", "dp", None),
    )
    out_specs = (
        P("dp", "expert"),
        P("expert", "dp"),
        P("expert", "dp", None),
        P("expert", "dp", None),
        P("expert", None, "dp"),
    )
    return jax.shard_map(local, mesh=mesh, in_specs=in_specs, out_specs=out_specs, check_vma=False)
```

```python
import functools

import jax
import jax.numpy as jnp
from jax import lax
from jax.experimental import pallas as pl
from jax.experimental.pallas import tpu as pltpu
from jax.sharding import PartitionSpec as P

LANES = 128
MESH = pl.DeviceIdType.MESH


def bit_orders(shards):
    bits = [1 << k for k in range(shards.bit_length() - 1)]
    return bits, [bits[:1] + bits[1:], bits[:1] + bits[:0:-1]]


def span(bits):
    found = [0]
    for bit in bits:
        found = found + [r | bit for r in found]
    return found


def entry_barrier(experts, bits):
    e = lax.axis_index("expert")
    d = lax.axis_index("dp")
    barrier = pltpu.get_barrier_semaphore()
    for k in range(1, experts):
        pl.semaphore_signal(barrier, inc=1, device_id={"expert": lax.rem(e + k, experts)}, device_id_type=MESH)
    for bit in bits:
        pl.semaphore_signal(barrier, inc=1, device_id={"dp": d ^ bit}, device_id_type=MESH)
    pl.semaphore_wait(barrier, experts - 1 + len(bits))


def dispatch_kernel(
    experts, shards, g_ref, i_ref, gate_ref, compact_ref, w_ref, ibuf, packed, raw, gbuf, wbuf, loc, a2a_s, a2a_r, ag_s, ag_r
):
    e = lax.axis_index("expert")
    d = lax.axis_index("dp")
    wd = g_ref.shape[2]
    width = wd * experts
    half = width // 2
    bits, orders = bit_orders(shards)
    entry_barrier(experts, bits)
    kinds = ((g_ref, gbuf), (i_ref, ibuf))

    def cols(src):
        return pl.ds(pl.multiple_of(src * wd, LANES), wd)

    def exchange(kind, k):
        ref, buf = kinds[kind]
        return pltpu.make_async_remote_copy(
            src_ref=ref.at[lax.rem(e + k, experts)],
            dst_ref=buf.at[d, :, cols(e)],
            send_sem=a2a_s.at[kind, k],
            recv_sem=a2a_r.at[kind, k],
            device_id={"expert": lax.rem(e + k, experts)},
            device_id_type=MESH,
        )

    def arrival(kind, k):
        ref, buf = kinds[kind]
        src = lax.rem(e + experts - k, experts)
        return pltpu.make_async_remote_copy(
            src_ref=ref.at[src],
            dst_ref=buf.at[d, :, cols(src)],
            send_sem=a2a_s.at[kind, k],
            recv_sem=a2a_r.at[kind, k],
            device_id={"expert": src},
            device_id_type=MESH,
        )

    for kind in range(2):
        for k in range(1, experts):
            exchange(kind, k).start()
    locals_ = [
        pltpu.make_async_copy(g_ref.at[e], gbuf.at[d, :, cols(e)], loc.at[0]),
        pltpu.make_async_copy(i_ref.at[e], ibuf.at[d, :, cols(e)], loc.at[1]),
        pltpu.make_async_copy(gate_ref, gbuf.at[d, :, pl.ds(width, LANES)], loc.at[2]),
    ]
    for c in locals_:
        c.start()
    weights = pltpu.make_async_copy(w_ref, wbuf, loc.at[3])
    weights.start()
    streams = []
    for kind in range(2):
        buf = kinds[kind][1]
        ends = (half, buf.shape[2] - half)
        for part in range(2):
            order = orders[part][1:] + orders[part][:1]
            streams.append((buf, pl.ds(part * half, ends[part]), order))

    def piece(n, r, t):
        buf, cut, order = streams[n]
        block = buf.at[d ^ r, :, cut]
        return pltpu.make_async_remote_copy(
            src_ref=block,
            dst_ref=block,
            send_sem=ag_s.at[n, r | order[t]],
            recv_sem=ag_r.at[n, r | order[t]],
            device_id={"dp": d ^ order[t]},
            device_id_type=MESH,
        )

    def landed(n, r):
        buf, cut, order = streams[n]
        block = buf.at[d ^ r, :, cut]
        return pltpu.make_async_remote_copy(
            src_ref=block,
            dst_ref=block,
            send_sem=ag_s.at[n, r],
            recv_sem=ag_r.at[n, r],
            device_id={"dp": d ^ order[0]},
            device_id_type=MESH,
        )

    started = []

    def forward(n, r, first):
        for t in range(first, len(bits)):
            piece(n, r, t).start()
            started.append((n, r, t))

    def begin(kind):
        locals_[kind].wait()
        for k in range(1, experts):
            arrival(kind, k).wait_recv()
        for part in range(2):
            forward(2 * kind + part, 0, 0)

    def receive(t, chosen_streams):
        for n in chosen_streams:
            order = streams[n][2]
            for r in span(order[:t]):
                got = r | order[t]
                landed(n, got).wait_recv()
                forward(n, got, t + 1)

    rows = compact_ref.shape[1] // 2

    def pack(tile, carry):
        cut = pl.ds(pl.multiple_of(tile * rows, rows), rows)
        total = jnp.dot(compact_ref[0, cut, :], gbuf[0], preferred_element_type=jnp.float32)
        for q in range(1, shards):
            total += jnp.dot(compact_ref[q, cut, :], gbuf[q], preferred_element_type=jnp.float32)
        packed[cut, :] = total.astype(jnp.bfloat16)
        return carry

    def multiply(tile, carry):
        cut = pl.ds(pl.multiple_of(tile * rows, rows), rows)
        raw[cut, :] = lax.dot_general(
            packed[cut, 0:width], wbuf[...], (((1,), (1,)), ((), ())), preferred_element_type=jnp.float32
        )
        return carry

    locals_[2].wait()
    begin(0)
    receive(0, (0, 1))
    begin(1)
    for t in range(1, len(bits) - 1):
        receive(t, (0, 1))
    receive(0, (2, 3))
    receive(len(bits) - 1, (0, 1))
    lax.fori_loop(0, 2, pack, 0)
    for t in range(1, len(bits) - 1):
        receive(t, (2, 3))
    weights.wait()
    lax.fori_loop(0, 2, multiply, 0)
    receive(len(bits) - 1, (2, 3))
    for n, r, t in started:
        piece(n, r, t).wait_send()
    for kind in range(2):
        for k in range(1, experts):
            exchange(kind, k).wait_send()


def return_kernel(experts, shards, dx_ref, dots_ref, gate_ref, obuf, own_ref, ra, rb, rd, sbuf, sem_s, sem_r, a2a_s, a2a_r):
    e = lax.axis_index("expert")
    d = lax.axis_index("dp")
    width = dx_ref.shape[2]
    half = width // 2
    wd = width // experts
    bits, orders = bit_orders(shards)
    entry_barrier(experts, bits)
    streams = (
        (dx_ref, pl.ds(0, half), orders[0], ra),
        (dx_ref, pl.ds(half, half), orders[1], rb),
        (dots_ref, pl.ds(0, LANES), orders[0], rd),
    )
    steps = len(bits)

    def slot(n, t, r):
        order = streams[n][2]
        before = sum(1 << (steps - 1 - q) for q in range(t))
        return before + span(order[t + 1 :]).index(r)

    def held(n, t, r):
        src, cut, order, buf = streams[n]
        if t == 0:
            return src.at[d ^ r, :, cut]
        return buf.at[slot(n, t - 1, r)]

    def piece(n, t, r):
        src, cut, order, buf = streams[n]
        place = slot(n, t, r)
        return pltpu.make_async_remote_copy(
            src_ref=held(n, t, r | order[t]),
            dst_ref=buf.at[place],
            send_sem=sem_s.at[n, place],
            recv_sem=sem_r.at[n, place],
            device_id={"dp": d ^ order[t]},
            device_id_type=MESH,
        )

    for r_index in range(1 << (steps - 1)):
        for n in range(3):
            order = streams[n][2]
            r = list(reversed(span(order[1:])))[r_index]
            piece(n, 0, r).start()
    finals = [None] * 3
    for t in range(steps):
        for r_index in range(1 << (steps - 1 - t)):
            for n in range(3):
                src, cut, order, buf = streams[n]
                r = list(reversed(span(order[t + 1 :])))[r_index]
                piece(n, t, r).wait_recv()
                place = slot(n, t, r)
                total = held(n, t, r)[...].astype(jnp.float32) + buf[place].astype(jnp.float32)
                if t == steps - 1:
                    finals[n] = total
                    if n < 2:
                        per = half // wd
                        for q in range(per):
                            sbuf[n * per + q, :, 0:wd] = total[:, q * wd : (q + 1) * wd].astype(jnp.bfloat16)
                else:
                    buf[place] = total.astype(jnp.bfloat16)
                    if r & order[t + 1]:
                        piece(n, t + 1, r ^ order[t + 1]).start()
    dots = finals[2]
    own_ref[...] = dots
    weighted = dots * gate_ref[...]
    high = weighted.astype(jnp.bfloat16)
    low = (weighted - high.astype(jnp.float32)).astype(jnp.bfloat16)
    lane = lax.broadcasted_iota(jnp.int32, high.shape, 1)
    extra = jnp.where(lane == 0, high.astype(jnp.float32), low.astype(jnp.float32)).astype(jnp.bfloat16)
    for q in range(experts):
        sbuf[q, :, wd : wd + LANES] = extra

    def exchange(k):
        to = lax.rem(e + k, experts)
        return pltpu.make_async_remote_copy(
            src_ref=sbuf.at[to],
            dst_ref=obuf.at[e],
            send_sem=a2a_s.at[k],
            recv_sem=a2a_r.at[k],
            device_id={"expert": to},
            device_id_type=MESH,
        )

    def arrival(k):
        src = lax.rem(e + experts - k, experts)
        return pltpu.make_async_remote_copy(
            src_ref=sbuf.at[src],
            dst_ref=obuf.at[src],
            send_sem=a2a_s.at[k],
            recv_sem=a2a_r.at[k],
            device_id={"expert": src},
            device_id_type=MESH,
        )

    for k in range(1, experts):
        exchange(k).start()
    obuf[e] = sbuf[e]
    for k in range(1, experts):
        arrival(k).wait_recv()
    for k in range(1, experts):
        exchange(k).wait_send()
    for n in range(3):
        for t in range(steps):
            for r in span(streams[n][2][t + 1 :]):
                piece(n, t, r).wait_send()


VMEM = pl.BlockSpec(memory_space=pltpu.VMEM)


def dispatch(experts, shards, sent_grad, sent_input, gate_rows, compact, weights):
    _, cap, wd = sent_grad.shape
    width = experts * wd
    return pl.pallas_call(
        functools.partial(dispatch_kernel, experts, shards),
        out_shape=(
            jax.ShapeDtypeStruct((shards, cap, width), jnp.bfloat16),
            jax.ShapeDtypeStruct((compact.shape[1], width + LANES), jnp.bfloat16),
            jax.ShapeDtypeStruct((compact.shape[1], weights.shape[0]), jnp.float32),
        ),
        in_specs=[VMEM] * 4 + [pl.BlockSpec(memory_space=pl.ANY)],
        out_specs=(VMEM, VMEM, VMEM),
        scratch_shapes=[
            pltpu.VMEM((shards, cap, width + LANES), jnp.bfloat16),
            pltpu.VMEM(weights.shape, jnp.bfloat16),
            pltpu.SemaphoreType.DMA((4,)),
            pltpu.SemaphoreType.DMA((2, experts)),
            pltpu.SemaphoreType.DMA((2, experts)),
            pltpu.SemaphoreType.DMA((4, shards)),
            pltpu.SemaphoreType.DMA((4, shards)),
        ],
        compiler_params=pltpu.CompilerParams(collective_id=0, has_side_effects=True),
        name="dispatch",
    )(sent_grad, sent_input, gate_rows, compact, weights)


def give_back(experts, shards, dx, dots, gate_rows):
    _, cap, width = dx.shape
    wd = width // experts
    return pl.pallas_call(
        functools.partial(return_kernel, experts, shards),
        out_shape=(
            jax.ShapeDtypeStruct((experts, cap, wd + LANES), jnp.bfloat16),
            jax.ShapeDtypeStruct((cap, LANES), jnp.float32),
        ),
        in_specs=[VMEM] * 3,
        out_specs=(VMEM, VMEM),
        scratch_shapes=[
            pltpu.VMEM((shards - 1, cap, width // 2), jnp.bfloat16),
            pltpu.VMEM((shards - 1, cap, width // 2), jnp.bfloat16),
            pltpu.VMEM((shards - 1, cap, LANES), jnp.bfloat16),
            pltpu.VMEM((experts, cap, wd + LANES), jnp.bfloat16),
            pltpu.SemaphoreType.DMA((3, shards)),
            pltpu.SemaphoreType.DMA((3, shards)),
            pltpu.SemaphoreType.DMA((experts,)),
            pltpu.SemaphoreType.DMA((experts,)),
        ],
        compiler_params=pltpu.CompilerParams(collective_id=1, has_side_effects=True),
        name="give_back",
    )(dx, dots, gate_rows)


def dot_t(a, b):
    return lax.dot_general(a, b, (((0,), (0,)), ((), ())), preferred_element_type=jnp.float32)


def local(grad_out, saved_inputs, router_probs, chosen, gate_pre, up_pre, w_down, w_up):
    tok_dev, wd = grad_out.shape
    shards = lax.axis_size("dp")
    shard_index = lax.axis_index("dp")
    expert = lax.axis_index("expert")
    experts, slots = chosen.shape
    cap = 3 * slots // (2 * shards)
    width = wd * experts
    bf16 = jnp.bfloat16
    owners = chosen // tok_dev
    firsts = jnp.sum((owners < shard_index).astype(jnp.int32), axis=1)
    slot_iota = jnp.arange(slots, dtype=jnp.int32)
    place = slot_iota[None, :] - firsts[:, None]
    place = jnp.where(owners == shard_index, place, -1)
    hit = place[:, None, :] == jnp.arange(cap, dtype=jnp.int32)[None, :, None]
    local_rows = jnp.max(jnp.where(hit, (chosen - shard_index * tok_dev)[:, None, :], -1), axis=2)
    token_iota = jnp.arange(tok_dev, dtype=jnp.int32)
    picker = (local_rows.reshape(-1)[:, None] == token_iota[None, :]).astype(bf16)
    sent_grad = jnp.dot(picker, grad_out, preferred_element_type=jnp.float32).astype(bf16)
    sent_input = jnp.dot(picker, saved_inputs, preferred_element_type=jnp.float32).astype(bf16)
    own_rows = lax.dynamic_index_in_dim(local_rows, expert, 0, keepdims=False)
    probs = router_probs[0]
    own_hit = own_rows[:, None] == token_iota[None, :]
    gate_own = jnp.sum(jnp.where(own_hit, probs[None, :], 0.0), axis=1)
    gate_wide = jnp.broadcast_to(gate_own[:, None], (cap, LANES))
    rows_all = shards * cap
    chosen_row = lax.dynamic_index_in_dim(chosen, expert, 0, keepdims=False)
    row_owner = chosen_row // tok_dev
    before = jnp.sum((row_owner[None, :] < row_owner[:, None]).astype(jnp.int32), axis=1)
    slot_place = row_owner * cap + slot_iota - before
    compact = (slot_place[:, None] == jnp.arange(rows_all, dtype=jnp.int32)[None, :]).astype(bf16)
    padded = jnp.arange(rows_all, dtype=jnp.int32).reshape(shards, 1, cap)
    blocks = (slot_place[None, :, None] == padded).astype(bf16)
    ibuf, packed, raw_grad = dispatch(
        experts,
        shards,
        sent_grad.reshape(experts, cap, wd),
        sent_input.reshape(experts, cap, wd),
        gate_wide.astype(bf16),
        blocks,
        w_down[0],
    )
    ibuf = ibuf.reshape(rows_all, width)
    dout = packed[:, :width]
    gate_slot = packed[:, width:][:, :1]
    gate_value = gate_pre[0].astype(jnp.float32)
    up_value = up_pre[0].astype(jnp.float32)
    sig = jax.nn.sigmoid(gate_value)
    active = gate_value * sig
    hidden = active * up_value
    dots = jnp.sum(hidden * raw_grad, axis=1)
    hid_grad = gate_slot.astype(jnp.float32) * raw_grad
    up_grad = (hid_grad * active).astype(bf16)
    gate_grad = (hid_grad * up_value * sig * (1.0 + gate_value * (1.0 - sig))).astype(bf16)
    up_pad = dot_t(compact, up_grad).astype(bf16)
    dx = jnp.dot(up_pad, w_up[0], preferred_element_type=jnp.float32).astype(bf16)
    dots_wide = jnp.broadcast_to(dots.astype(bf16)[:, None], (slots, LANES))
    dots_pad = dot_t(compact, dots_wide).astype(bf16)
    grad_down = dot_t(hidden.astype(bf16), gate_slot * dout).astype(bf16)
    grad_up = dot_t(up_pad, ibuf).astype(bf16)
    spread, dots_own = give_back(
        experts, shards, dx.reshape(shards, cap, width), dots_pad.reshape(shards, cap, LANES), gate_wide
    )
    spread = spread.reshape(experts * cap, wd + LANES)
    summed = dot_t(picker, spread)
    grad_tokens = summed[:, :wd].astype(bf16)
    router_sum = summed[:, wd] + summed[:, wd + 1]
    gate_tokens = jnp.sum(jnp.where(own_hit, dots_own[:, :1], 0.0), axis=0)
    grad_logits = (probs * (gate_tokens - router_sum))[None, :]
    return grad_tokens, grad_logits, grad_down[None], grad_up[None], gate_grad[None]


def solution(mesh):
    in_specs = (
        P("dp", "expert"),
        P("dp", "expert"),
        P("expert", "dp"),
        P(),
        P("expert", None, "dp"),
        P("expert", None, "dp"),
        P("expert", "dp", None),
        P("expert", "dp", None),
    )
    out_specs = (
        P("dp", "expert"),
        P("expert", "dp"),
        P("expert", "dp", None),
        P("expert", "dp", None),
        P("expert", None, "dp"),
    )
    return jax.shard_map(local, mesh=mesh, in_specs=in_specs, out_specs=out_specs, check_vma=False)
```
